32 devices in a mesh: vocab: 4 (over x, core), expert: 8 (over z, y).
Axes of the slice: x: 2, y: 2, z: 4, core: 2. Of those that a mesh axis runs over, the one named last changes fastest.
Arguments:
- leading_batch_features: bfloat16 [256, 2880], P(('vocab', 'expert')), may hold values from -48 to 48
- sampling_heat_selector: int32 [256], replicated, may hold values from 0 to 3
- output_embedding_matrix: bfloat16 [50272, 2880], P(('vocab', 'expert')), may hold values from -3.354102 to 3.354102
- trailing_batch_features: bfloat16 [512, 2880], P('expert'), may hold values from -6 to 6
- routed_specialist_choice: int32 [512, 4], P('expert'), may hold values from 0 to 31, all different within a row; in each aligned block of 64 rows (0 to 63, 64 to 127, ...) at most 16 rows name the same one
- dispatcher_projection: bfloat16 [2880, 32], replicated, may hold values from -13.416408 to 13.416408
- specialist_gating_matrix: bfloat16 [32, 2880, 1440], P('expert', None, 'vocab'), may hold values from -0.109375 to 0.109375
- specialist_raising_matrix: bfloat16 [32, 2880, 1440], P('expert', None, 'vocab'), may hold values from -0.109375 to 0.109375
- expert_lowering_matrix: bfloat16 [32, 1440, 2880], P('expert', 'vocab'), may hold values from -0.15625 to 0.15625
Outputs:
- lexicon_log_probability: float32 [256, 50272], P(None, ('vocab', 'expert'))
- moe_out: bfloat16 [512, 2880], P('expert', 'vocab')
The draws below stay inside these ranges and needn't reach their ends.
Inputs may be any that keep to these rules, and one draw needn't show every extreme that they name: `routed_specialist_choice`: in the rows of one index of the expert axis no expert is named more than 16 times, a bound that some block reaches.
All inputs are finite; a program needn't handle non-finite values.
Results may differ from the reference program's by a relative error of at most 0.005.
The reference program's roundings to bfloat16 on the way count: a program that leaves them out, or rounds other values in their place, can miss the bound.
Values may be sent and summed in bfloat16 or wider, within the bound.
A program may use at most 256 MiB of HBM per device.

```python
import math
import jax
import jax.numpy as jnp
import numpy as np
from jax import lax

EMBED_DIMENSION = 2880
FF = 1440
TOPK = 4
TB_DEV = 64
EXPERTS = 32
VOCAB = 50272
LEAD_BATCH_SIZE = 256
TB = 512
CAP = 16
N_EXPERT = 8


def draw_leading_batch_features(key, part):
    key_base = jax.random.fold_in(jax.random.fold_in(key, 11), 0)
    normal_part = jnp.clip(jax.random.normal(key_base, (LEAD_BATCH_SIZE, EMBED_DIMENSION), jnp.float32), -6.0, 6.0)
    return normal_part.astype(jnp.bfloat16)


def draw_output_embedding_matrix(key, part):
    key_base, key_scale = jax.random.split(jax.random.fold_in(key, 23))
    normal_part = jnp.clip(jax.random.normal(key_base, (VOCAB, EMBED_DIMENSION), jnp.float32), -6.0, 6.0) * EMBED_DIMENSION ** (-0.5)
    frac_rows = (jnp.arange(VOCAB, dtype=jnp.float32) / VOCAB)[:, None]
    row_scale = 2.0 * jnp.exp(frac_rows * jnp.log(3.0) + jax.random.uniform(key_scale, (VOCAB, 1), jnp.float32, -0.7, 0.7))
    return (normal_part * row_scale).astype(jnp.bfloat16)


def draw_dispatcher_projection(key, part):
    key_base = jax.random.fold_in(jax.random.fold_in(key, 37), 0)
    normal_part = jnp.clip(jax.random.normal(key_base, (EMBED_DIMENSION, EXPERTS), jnp.float32), -6.0, 6.0) * 2.0 * EMBED_DIMENSION ** (-0.5)
    return normal_part.astype(jnp.bfloat16)


def place_ends(result, stream_key, low, top_value):
    spot = [jax.random.randint(jax.random.fold_in(stream_key, axis), (), 0, length) for axis, length in enumerate(result.shape)]
    longest = result.shape.index(max(result.shape))
    beside = spot[:longest] + [(spot[longest] + 1) % result.shape[longest]] + spot[longest + 1:]
    return result.at[tuple(spot)].set(low).at[tuple(beside)].set(top_value)


def level_of(stream_key, extent, cuts, low, largest):
    loudness, own = 1.0, jax.random.fold_in(stream_key, 6)
    for axis_at, blocks in cuts:
        draws = jnp.exp(jax.random.uniform(jax.random.fold_in(own, axis_at), (blocks,), jnp.float32, low / len(cuts), largest / len(cuts)))
        loudness = loudness * jnp.repeat(draws, extent[axis_at] // blocks).reshape([-1 if axis == axis_at else 1 for axis in range(len(extent))])
    return loudness


def deal_out(rng, own, number, rows, number_of, top, most, lean):
    sequence = jax.random.permutation(rng, number_of)
    heavy_load, common = shares(number_of, rows * top, most, lean, True), shares(number_of, rows * top, most, lean, False)
    places = jnp.arange(number_of)

    def named(lengths, rotation):
        used = int((lengths > 0).sum())
        fixed = max(1, used // 4)
        shifted = fixed + (places - fixed + rotation * (used - fixed)) % max(1, number_of - fixed)
        return jnp.zeros((number_of,), jnp.int32).at[sequence[jnp.where(places < fixed, places, shifted)]].set(jnp.asarray(lengths, jnp.int32))

    lengths = jnp.where(number % 4 == 0, named(heavy_load, number // 4), named(common, number - number // 4 - 1))
    mixed = jax.random.permutation(jax.random.fold_in(own, 3), number_of)
    source_of, receiver = mixed[0:number_of // 2 * 2:2], mixed[1:number_of // 2 * 2:2]
    slack = jnp.minimum(lengths[source_of] - 1, most - lengths[receiver]) // 2
    slack = jnp.where((source_of == sequence[0]) | (receiver == sequence[0]) | (lengths[receiver] == 0), 0, jnp.maximum(slack, 0))
    shifted = jax.random.randint(jax.random.fold_in(own, 4), (number_of // 2,), 0, 1 << 20) % (slack + 1)
    lengths = lengths.at[source_of].add(-shifted).at[receiver].add(shifted)
    items = jnp.searchsorted(jnp.cumsum(lengths), jnp.arange(rows * top), side="right").astype(jnp.int32)
    listing = items.reshape(top, rows).T
    listing = listing[jax.random.permutation(jax.random.fold_in(own, 1), rows)]
    rotation = jax.random.randint(jax.random.fold_in(own, 2), (rows, 1), 0, top)
    return jnp.take_along_axis(listing, (jnp.arange(top)[None, :] + rotation) % top, axis=1)


def shares(number_of, total, reach, slope, full):
    weights = [(1 << 20) // math.isqrt(grade ** slope) + 1 for grade in range(1, number_of + 1)]
    largest = reach if full else min(reach, max(-(-total // number_of), total * weights[0] // sum(weights)))
    least = 1 if total - largest >= number_of - 1 else 0
    given, surplus = [largest] + [least] * (number_of - 1), total - largest - least * (number_of - 1)
    while surplus > 0:
        candidates = [i for i in range(1, number_of) if given[i] < largest] or [i for i in range(1, number_of) if given[i] < reach]
        whole, left = sum([weights[i] for i in candidates]), surplus
        for i in candidates:
            addition = min(reach - given[i], max(1, left * weights[i] // whole), surplus)
            given[i] = given[i] + addition
            surplus = surplus - addition
    return np.array(given)


def noise(own_key, extent, spread, limit, pieces=(), kind=jnp.bfloat16):
    level = level_of(own_key, extent, pieces, -0.22, 0.18) if pieces else 1.0
    entries = jax.random.normal(own_key, extent, jnp.float32) * spread * level
    return jnp.minimum(jnp.maximum(entries, -limit), limit).astype(kind)


def setup_inputs(seed: int = 0) -> dict:
    streams_of = jax.random.split(jax.random.key(seed), 10)
    leading_batch_features = draw_leading_batch_features(jax.random.fold_in(streams_of[9], 71), 0)
    sampling_heat_selector = place_ends(jax.random.randint(streams_of[1], (LEAD_BATCH_SIZE,), 0, 4), jax.random.fold_in(streams_of[1], 1), 0, 3).astype(jnp.int32)
    output_embedding_matrix = draw_output_embedding_matrix(jax.random.fold_in(streams_of[9], 71), 0)
    trailing_batch_features = noise(streams_of[3], (TB, EMBED_DIMENSION), 1.0, 6.0, ((0, 8),))
    routed_specialist_choice_keys = jax.random.split(jax.random.fold_in(streams_of[4], 1), TB // TB_DEV)
    routed_specialist_choice_turns = jax.random.permutation(jax.random.fold_in(streams_of[4], 3), TB // TB_DEV)
    routed_specialist_choice = jax.vmap(lambda own, number: deal_out(jax.random.fold_in(streams_of[4], 2), own, number, TB_DEV, EXPERTS, TOPK, CAP, 2))(routed_specialist_choice_keys, routed_specialist_choice_turns).reshape((TB, TOPK))
    dispatcher_projection = draw_dispatcher_projection(jax.random.fold_in(streams_of[9], 71), 0)
    specialist_gating_matrix = noise(streams_of[6], (EXPERTS, EMBED_DIMENSION, FF), EMBED_DIMENSION ** -0.5, 0.109375, ((0, 8), (2, 4)))
    specialist_raising_matrix = noise(streams_of[7], (EXPERTS, EMBED_DIMENSION, FF), EMBED_DIMENSION ** -0.5, 0.109375, ((0, 8), (2, 4)))
    expert_lowering_matrix = noise(streams_of[8], (EXPERTS, FF, EMBED_DIMENSION), FF ** -0.5, 0.15625, ((0, 8), (1, 4)))
    return dict(leading_batch_features=leading_batch_features, sampling_heat_selector=sampling_heat_selector, output_embedding_matrix=output_embedding_matrix, trailing_batch_features=trailing_batch_features, routed_specialist_choice=routed_specialist_choice, dispatcher_projection=dispatcher_projection, specialist_gating_matrix=specialist_gating_matrix, specialist_raising_matrix=specialist_raising_matrix, expert_lowering_matrix=expert_lowering_matrix)


def slot_numbers(flat_ids, expert_count):
    one_hot = (flat_ids[:, None] == jnp.arange(expert_count, dtype=jnp.int32)[None, :]).astype(jnp.int32)
    earlier = jnp.cumsum(one_hot, axis=0) - one_hot
    return jnp.sum(earlier * one_hot, axis=1).astype(jnp.int32)


def reference(leading_batch_features, sampling_heat_selector, output_embedding_matrix, trailing_batch_features, routed_specialist_choice, dispatcher_projection, specialist_gating_matrix, specialist_raising_matrix, expert_lowering_matrix):
    lexicon_piece_number = math.gcd(LEAD_BATCH_SIZE, 64)
    position_heat_factor = 0.5 + 0.25 * sampling_heat_selector.astype(jnp.float32)

    def lexicon_score_piece(operands):
        token_rows, row_temps = operands
        plain_lexicon_scores = lax.dot_general(token_rows, output_embedding_matrix, (((1,), (1,)), ((), ())), preferred_element_type=jnp.float32)
        heat_divided_scores = plain_lexicon_scores / row_temps[:, None]
        row_max = jnp.max(heat_divided_scores, axis=1)
        row_total = jnp.sum(jnp.exp(heat_divided_scores - row_max[:, None]), axis=1)
        return heat_divided_scores - row_max[:, None] - jnp.log(row_total)[:, None]

    lexicon_log_probability = lax.map(lexicon_score_piece, (leading_batch_features.reshape(LEAD_BATCH_SIZE // lexicon_piece_number, lexicon_piece_number, EMBED_DIMENSION), position_heat_factor.reshape(LEAD_BATCH_SIZE // lexicon_piece_number, lexicon_piece_number)))
    lexicon_log_probability = lexicon_log_probability.reshape(LEAD_BATCH_SIZE, VOCAB)

    router_full = jnp.dot(trailing_batch_features, dispatcher_projection, preferred_element_type=jnp.float32)
    scores = jnp.take_along_axis(router_full, routed_specialist_choice, axis=1)
    gate_probs = jax.nn.softmax(scores, axis=1)
    slots = jax.vmap(lambda ids_block: slot_numbers(ids_block, EXPERTS))(routed_specialist_choice.reshape(N_EXPERT, TB_DEV * TOPK))
    slots = slots.reshape(TB, TOPK)
    block_index = (jnp.arange(TB, dtype=jnp.int32) // TB_DEV).astype(jnp.int32)
    slot_index = (routed_specialist_choice * (N_EXPERT * CAP) + block_index[:, None] * CAP + slots).reshape(-1).astype(jnp.int32)
    token_rows = jnp.repeat(trailing_batch_features, TOPK, axis=0)
    buffer = jnp.zeros((EXPERTS * N_EXPERT * CAP, EMBED_DIMENSION), jnp.bfloat16).at[slot_index].set(token_rows)
    buffer = buffer.reshape(EXPERTS, N_EXPERT * CAP, EMBED_DIMENSION)

    def one_expert(operands):
        expert_rows, w_gate, w_up, w_down = operands
        gate_proj = jnp.dot(expert_rows, w_gate, preferred_element_type=jnp.float32)
        up_proj = jnp.dot(expert_rows, w_up, preferred_element_type=jnp.float32)
        activated = (gate_proj * jax.nn.sigmoid(1.702 * gate_proj) * (up_proj + 1.0)).astype(jnp.bfloat16)
        return jnp.dot(activated, w_down, preferred_element_type=jnp.float32).astype(jnp.bfloat16)

    expert_outs = lax.map(one_expert, (buffer, specialist_gating_matrix, specialist_raising_matrix, expert_lowering_matrix))
    expert_outs = expert_outs.reshape(EXPERTS * N_EXPERT * CAP, EMBED_DIMENSION)
    picked = expert_outs[slot_index].reshape(TB, TOPK, EMBED_DIMENSION).astype(jnp.float32)
    moe_out = jnp.sum(gate_probs[:, :, None] * picked, axis=1).astype(jnp.bfloat16)
    return lexicon_log_probability, moe_out
```

```python
import functools

import jax
import jax.numpy as jnp
from jax import lax
from jax.experimental import pallas as pl
from jax.experimental.pallas import tpu as pltpu
from jax.sharding import PartitionSpec as P

MESH = pl.DeviceIdType.MESH
ANY = pl.BlockSpec(memory_space=pl.ANY)
VMEM = pl.BlockSpec(memory_space=pltpu.VMEM)
CORES = 2
UNIT = 8
F32 = jnp.float32
BF16 = jnp.bfloat16


def dot_nt(a, b):
    return lax.dot_general(a, b, (((1,), (1,)), ((), ())), preferred_element_type=F32)


def body(
    dims,
    lead_ref, heat_ref, embed_ref, tok_ref, choice_ref, router_ref, wg_ref, wu_ref, wd_ref,
    sc_ref, norm_ref, moe_ref,
    embed_v, wg_v, wu_v, wd_raw, wd_v, xblk, lead_v, heat_v, choice_v, router_v, ptile, held, x2, pcol,
    act, logits, s_send, s_own, s_recv, sb3, rb3, sb2, rb2, sbz, rbz, acc, stat_mine, stat_all,
    sem_small, sem_l, sem_w, sem_raw, gs, gr, sem_ss, sem_sr, s3s, s3r, s2s, s2r, szs, szr, st_s, st_r,
):
    nv, ne, nx, na, nb = dims
    n = nv * ne
    v = lax.axis_index("vocab")
    e = lax.axis_index("expert")
    x, c = v // CORES, lax.rem(v, CORES)
    a, b = e // nb, lax.rem(e, nb)
    n1, n2, n3 = na, nb, nx
    if nx == nb:
        p2 = jnp.where(c == 0, b, x)
        p3 = jnp.where(c == 0, x, b)
    else:
        p2, p3 = b, x

    def dev(a_, p2_, p3_, c_):
        if nx == nb:
            b_ = jnp.where(c == 0, p2_, p3_)
            x_ = jnp.where(c == 0, p3_, p2_)
        else:
            b_, x_ = p2_, p3_
        return (x_ * CORES + c_, a_ * nb + b_)

    def wrap(i, size):
        return jnp.where(i >= size, i - size, i)

    groups = held.shape[0]
    nq = groups - 1

    def near(da, d2, d3):
        return wrap(a + da, n1), wrap(p2 + d2, n2), wrap(p3 + d3, n3)

    def others(act_on):
        for dv in range(nv):

            @pl.loop(0 if dv else 1, ne)
            def _(de):
                act_on(wrap(v + dv, nv), wrap(e + de, ne), dv * ne + de)

    def slot(g, a_, p2_, p3_, c_):
        v_, e_ = dev(a_, p2_, p3_, c_)
        return v_ * ne + e_ if g == nq else e_ * nv + v_

    me = e * nv + v
    width = xblk.shape[2]
    nexp = router_v.shape[0]
    local, ff, _ = wg_v.shape
    raw_depth = wd_raw.shape[0]
    span = wd_v.shape[3]
    rows = xblk.shape[0] * UNIT

    small = [
        pltpu.make_async_copy(tok_ref, xblk, sem_small.at[0]),
        pltpu.make_async_copy(choice_ref, choice_v, sem_small.at[1]),
        pltpu.make_async_copy(router_ref, router_v, sem_small.at[2]),
        pltpu.make_async_copy(heat_ref, heat_v, sem_small.at[3]),
        pltpu.make_async_copy(lead_ref, lead_v, sem_small.at[4]),
    ]
    raw = [pltpu.make_async_copy(wd_ref.at[l], wd_raw.at[l % raw_depth], sem_raw.at[l]) for l in range(local)]
    wg_in = [pltpu.make_async_copy(wg_ref.at[l], wg_v.at[l], sem_w.at[0, l]) for l in range(local)]
    wu_in = [pltpu.make_async_copy(wu_ref.at[l], wu_v.at[l], sem_w.at[1, l]) for l in range(local)]
    depth, tile = logits.shape[0], logits.shape[1]
    vocab = embed_ref.shape[0]
    tiles = -(-vocab // tile)

    def extent(t):
        return t * tile, min(tile, vocab - t * tile)

    def sc_out(t):
        at = t * tile
        return pltpu.make_async_copy(
            logits.at[t % depth], sc_ref.at[at : at + tile], sem_l.at[t]
        )

    embed_in = pltpu.make_async_copy(embed_ref, embed_v, sem_small.at[5])

    for copy in small:
        copy.start()

    barrier = pltpu.get_barrier_semaphore()

    def greet(v_, e_, k):
        pl.semaphore_signal(barrier, inc=1, device_id=(v_, e_), device_id_type=MESH)

    others(greet)

    for l in range(min(raw_depth, local)):
        raw[l].start()
    for l in range(local):
        wg_in[l].start()
        wu_in[l].start()
    embed_in.start()

    for copy in small:
        copy.wait()
    scores = dot_nt(router_v[...], xblk[...].reshape(rows, width))
    ids = choice_v[...]
    expert = lax.broadcasted_iota(jnp.int32, (nexp, rows), 0)
    hot = expert == ids[0:1, :]
    for k in range(1, ids.shape[0]):
        hot = jnp.logical_or(hot, expert == ids[k : k + 1, :])
    peak = jnp.max(jnp.where(hot, scores, -jnp.inf), axis=0, keepdims=True)
    weight = jnp.where(hot, jnp.exp(jnp.where(hot, scores - peak, 0.0)), 0.0)
    prob = weight / jnp.sum(weight, axis=0, keepdims=True)
    high = prob.astype(BF16).astype(F32)
    ptile[...] = jnp.zeros_like(ptile)
    ptile[0:nexp, 0:rows] = high
    ptile[nexp : 2 * nexp, 0:rows] = prob - high
    ptile[...] = ptile[...].T
    for q in range(nq):
        unit = v * nq + q
        held[q, me, :, 0:width] = xblk[unit]
        start = pl.multiple_of(unit * UNIT, UNIT)
        held[q, me, :, width : width + 2 * nexp] = ptile[pl.ds(start, UNIT), 0 : 2 * nexp].astype(
            BF16
        )

    held[nq, v * ne + e, :, 0:width] = lead_v[...]

    pl.semaphore_wait(barrier, n - 1)

    base2 = n1 - 1
    base3 = base2 + (n2 - 1) * n1
    base_s = base3 + (n3 - 1) * n1 * n2

    def gcopy(g, s, k, target):
        return pltpu.make_async_remote_copy(
            src_ref=held.at[g, s],
            dst_ref=held.at[g, s],
            send_sem=gs.at[g, k],
            recv_sem=gr.at[g, s],
            device_id=target,
            device_id_type=MESH,
        )

    def forward(g, da, d2, d3, stage):
        s = slot(g, *near(da, d2, d3), c)
        if stage <= 1:
            for k2 in range(1, n2):
                gcopy(g, s, base2 + (k2 - 1) * n1 + da, dev(*near(0, k2, 0), c)).start()
        if stage <= 2:
            for k3 in range(1, n3):
                gcopy(g, s, base3 + ((k3 - 1) * n2 + d2) * n1 + da, dev(*near(0, 0, k3), c)).start()
        gcopy(g, s, base_s + (d3 * n2 + d2) * n1 + da, dev(a, p2, p3, 1 - c)).start()

    def arrive(g, s):
        gcopy(g, s, 0, dev(a, p2, p3, 1 - c)).wait_recv()

    def g_start(g):
        for d in range(1, n1):
            gcopy(g, slot(g, *near(0, 0, 0), c), d - 1, dev(*near(d, 0, 0), c)).start()
        forward(g, 0, 0, 0, 1)

    def g_one(g):
        @pl.loop(1, n1)
        def _(da):
            arrive(g, slot(g, *near(da, 0, 0), c))
            forward(g, da, 0, 0, 1)

    def g_two(g):
        for d2 in range(1, n2):

            @pl.loop(0, n1)
            def _(da):
                arrive(g, slot(g, *near(da, d2, 0), c))
                forward(g, da, d2, 0, 2)

    def g_three(g, d2s=None):
        for d2 in range(n2) if d2s is None else d2s:
            for d3 in range(1, n3):

                @pl.loop(0, n1)
                def _(da):
                    arrive(g, slot(g, *near(da, d2, d3), c))
                    forward(g, da, d2, d3, 3)

    def g_sib(g):
        for d3 in range(n3):
            for d2 in range(n2):

                @pl.loop(0, n1)
                def _(da):
                    arrive(g, slot(g, *near(da, d2, d3), 1 - c))

    def g_end(g):
        @pl.loop(0, n - 1)
        def _(k):
            gcopy(g, me, k, dev(a, p2, p3, 1 - c)).wait_send()

    def wd_shift(l):
        raw[l].wait()
        for w in range(nv):
            wd_v[l, w] = wd_raw[l % raw_depth, :, w * span : (w + 1) * span]
        if l + raw_depth < local:
            raw[l + raw_depth].start()

    def load_x(g):
        x2[...] = held[g, :, :, 0:width].reshape(n * UNIT, width)

    def load_p(q):
        tail = held[q, :, :, width : width + 2 * nexp].reshape(n * UNIT, 2 * nexp).astype(F32)
        lane = lax.rem(lax.broadcasted_iota(jnp.int32, tail.shape, 1), nexp)
        for l in range(local):
            pcol[:, l : l + 1] = jnp.sum(
                jnp.where(lane == e * local + l, tail, 0.0), axis=1, keepdims=True
            )

    def gate_up(l):
        gate = dot_nt(wg_v[l], x2[...])
        up = dot_nt(wu_v[l], x2[...])
        act[l] = (gate * jax.nn.sigmoid(1.702 * gate) * (up + 1.0)).astype(BF16).T

    def down(w):
        total = pcol[:, 0:1] * jnp.dot(act[0], wd_v[0, w], preferred_element_type=F32)
        for l in range(1, local):
            total += pcol[:, l : l + 1] * jnp.dot(act[l], wd_v[l, w], preferred_element_type=F32)
        return total.reshape(ne, n * UNIT // ne, span)

    def scopy(q, j):
        return pltpu.make_async_remote_copy(
            src_ref=s_send.at[q, j],
            dst_ref=s_recv.at[q, j],
            send_sem=sem_ss.at[q, j],
            recv_sem=sem_sr.at[q, j],
            device_id=dev(a, p2, p3, 1 - c),
            device_id_type=MESH,
        )

    def down_send(q):
        @pl.loop(0, nx)
        def _(j):
            s_send[q, j] = down(j * CORES + 1 - c).astype(s_send.dtype)
            scopy(q, j).start()

    def down_own(q):
        @pl.loop(0, nx)
        def _(j):
            s_own[q, j] = down(j * CORES + c).astype(s_own.dtype)

    def chip(q, a_, p2_, p3_):
        v_, e_ = dev(a_, p2_, p3_, c)
        x_ = v_ // CORES
        return s_own[q, x_, e_].astype(F32) + s_recv[q, x_, e_].astype(F32)

    shared = len(sb3.shape) == 2
    sb3 = s_send if shared else sb3

    def c3(q, d3, i, target):
        return pltpu.make_async_remote_copy(
            src_ref=sb3.at[q, d3 - 1, i],
            dst_ref=rb3.at[q, d3 - 1, i],
            send_sem=s3s.at[q, d3 - 1, i],
            recv_sem=s3r.at[q, d3 - 1, i],
            device_id=target,
            device_id_type=MESH,
        )

    def c2(q, d2, i, target):
        return pltpu.make_async_remote_copy(
            src_ref=sb2.at[q, d2 - 1, i],
            dst_ref=rb2.at[q, d2 - 1, i],
            send_sem=s2s.at[q, d2 - 1, i],
            recv_sem=s2r.at[q, d2 - 1, i],
            device_id=target,
            device_id_type=MESH,
        )

    def c1(q, d, target):
        return pltpu.make_async_remote_copy(
            src_ref=sbz.at[q, d - 1],
            dst_ref=rbz.at[q, d - 1],
            send_sem=szs.at[q, d - 1],
            recv_sem=szr.at[q, d - 1],
            device_id=target,
            device_id_type=MESH,
        )

    def c_send(q):
        @pl.loop(0, nx)
        def _(j):
            scopy(q, j).wait_recv()
            if shared:
                scopy(q, j).wait_send()

        for d3 in range(1, n3):

            for d2 in range(n2 - 1, -1, -1):

                @pl.loop(0, n1)
                def _(i):
                    a_, p2_, p3_ = near(wrap(i + 1, n1), d2, d3)
                    k = a_ * n2 + p2_
                    sb3[q, d3 - 1, k] = chip(q, a_, p2_, p3_).astype(BF16)
                    c3(q, d3, k, dev(*near(0, 0, d3), c)).start()

    def c_three(q):
        def total(da, d2):
            a_, p2_, p3_ = near(da, d2, 0)
            k = a_ * n2 + p2_
            part = chip(q, a_, p2_, p3_)
            for d3 in range(1, n3):
                c3(q, d3, k, dev(a, p2, p3, 1 - c)).wait_recv()
                part += rb3[q, d3 - 1, k].astype(F32)
            return a_, part

        for d2 in range(n2 - 1, 0, -1):

            @pl.loop(0, n1)
            def _(i):
                a_, part = total(wrap(i + 1, n1), d2)
                sb2[q, d2 - 1, a_] = part.astype(BF16)
                c2(q, d2, a_, dev(*near(0, d2, 0), c)).start()

        @pl.loop(0, n1)
        def _(i):
            a_, part = total(wrap(i + 1, n1), 0)
            acc[q, a_] = part

    def c_two(q):
        def total(a_):
            part = acc[q, a_]
            for d2 in range(1, n2):
                c2(q, d2, a_, dev(a, p2, p3, 1 - c)).wait_recv()
                part += rb2[q, d2 - 1, a_].astype(F32)
            return part

        @pl.loop(1, n1)
        def _(da):
            a_, p2_, p3_ = near(da, 0, 0)
            sbz[q, da - 1] = total(a_).astype(BF16)
            c1(q, da, dev(a_, p2_, p3_, c)).start()

        acc[q, a] = total(a)

    def c_one(q):
        part = acc[q, a]
        for d in range(1, n1):
            c1(q, d, dev(a, p2, p3, 1 - c)).wait_recv()
            part += rbz[q, d - 1].astype(F32)
        part = part.astype(BF16)
        for w in range(nv):
            at = (w * nq + q) * UNIT
            moe_ref[at : at + UNIT, :] = part[w * UNIT : (w + 1) * UNIT]

    def c_end(q):
        nobody = dev(a, p2, p3, 1 - c)

        if not shared:

            @pl.loop(0, nx)
            def _(j):
                scopy(q, j).wait_send()

        for d3 in range(1, n3):

            @pl.loop(0, n1 * n2)
            def _(i):
                c3(q, d3, i, nobody).wait_send()

        for d2 in range(1, n2):

            @pl.loop(0, n1)
            def _(i):
                c2(q, d2, i, nobody).wait_send()

        for d in range(1, n1):
            c1(q, d, nobody).wait_send()

    def lm_tile(t, top, total):
        at, size = extent(t)
        if t == 0:
            embed_in.wait()
        scale = 1.0 / (0.5 + 0.25 * heat_v[...].astype(F32))
        part = dot_nt(embed_v[at : at + size], x2[...]) * scale
        if t >= depth:
            sc_out(t - depth).wait()
        logits[t % depth, 0:size] = part
        sc_out(t).start()
        peak = jnp.maximum(top, jnp.max(part, axis=0, keepdims=True))
        total = total * jnp.exp(top - peak) + jnp.sum(jnp.exp(part - peak), axis=0, keepdims=True)
        return peak, total

    def stat(v_, e_, s, k):
        return pltpu.make_async_remote_copy(
            src_ref=stat_mine,
            dst_ref=stat_all.at[s],
            send_sem=st_s.at[k],
            recv_sem=st_r.at[s],
            device_id=(v_, e_),
            device_id_type=MESH,
        )

    def lm_send(top, total):
        stat_mine[0:1, :] = top
        stat_mine[1:2, :] = total
        stat_all[pl.ds(me, 1)] = stat_mine[...][None]
        others(lambda v_, e_, k: stat(v_, e_, me, k).start())

    def lm_end():
        others(lambda v_, e_, k: stat(v_, e_, e_ * nv + v_, k).wait())
        tops = stat_all[:, 0, :]
        top = jnp.max(tops, axis=0, keepdims=True)
        total = jnp.sum(stat_all[:, 1, :] * jnp.exp(tops - top), axis=0, keepdims=True)
        norm_ref[...] = top + jnp.log(total)
        for t in range(max(0, tiles - depth), tiles):
            sc_out(t).wait()

    last = nq
    for g in range(groups):
        g_start(g)
    g_one(0)
    wd_shift(0)
    g_two(0)
    if nq > 1:
        g_one(1)
    wd_shift(1)
    g_three(0)
    if nq > 1:
        g_two(1)
    g_one(last)
    g_sib(0)
    load_x(0)
    load_p(0)

    def during(q):
        steps = []
        if q + 1 < nq:
            steps += [lambda: g_three(q + 1, [0]), lambda: g_three(q + 1, range(1, n2))]
            if q + 2 < nq:
                steps += [lambda: g_one(q + 2), lambda: g_two(q + 2)]
        if q == 0:
            steps += [lambda: g_two(last)]
            steps += [lambda: g_three(last, [0]), lambda: g_three(last, range(1, n2))]
        if q:
            steps += [lambda: c_send(q - 1), lambda: c_three(q - 1)]
            steps += [lambda: c_two(q - 1), lambda: c_one(q - 1)]
        return steps

    for q in range(nq):
        if q:
            g_sib(q)
            load_x(q)
            load_p(q)
        steps = during(q)
        work = []
        for l in range(local):
            work.append(functools.partial(gate_up, l))
        work += [lambda: down_send(q), lambda: down_own(q)]
        for l, step in enumerate(work):
            if q == 0 and l < local:
                wg_in[l].wait()
                wu_in[l].wait()
                if l >= 2:
                    wd_shift(l)
            step()
            if steps:
                steps.pop(0)()
        for step in steps:
            step()
    q = nq - 1
    g_sib(last)
    load_x(last)
    steps = [lambda: c_send(q), lambda: c_three(q), lambda: c_two(q)]
    top, total = jnp.full((1, n * UNIT), -jnp.inf, F32), jnp.zeros((1, n * UNIT), F32)
    for t in range(tiles):
        if steps:
            steps.pop(0)()
        top, total = lm_tile(t, top, total)
    lm_send(top, total)
    for step in steps:
        step()
    c_one(q)
    lm_end()
    for g in range(groups):
        g_end(g)
    for q in range(nq):
        c_end(q)


def fused(dims, lead, heat, embed, tok, choice, router, wg, wu, wd):
    nv, ne, nx, na, nb = dims
    n = nv * ne
    local, ff, width = wg.shape
    vocab = embed.shape[0]
    rows = tok.shape[0] * UNIT
    nexp = router.shape[0]
    span = width // nv
    nq = tok.shape[0] // nv
    groups = nq + 1
    tokens = n * UNIT
    wide = -(-(width + 2 * nexp) // 128) * 128
    per = tokens // ne
    side = -(-max(2 * nexp, rows) // 128) * 128
    n1, n2, n3 = na, nb, nx
    roomy = 3 * nx * nq * tokens * (-(-span // 128) * 128) * 4 < 10 << 20
    tile = -(-vocab // (64 if roomy else 128)) * 16
    tiles = -(-vocab // tile)
    link, depth = (F32, tiles) if roomy else (BF16, 2)
    dma = pltpu.SemaphoreType.DMA
    scratch = [
        pltpu.VMEM((vocab, width), BF16),
        pltpu.VMEM((local, ff, width), BF16),
        pltpu.VMEM((local, ff, width), BF16),
        pltpu.VMEM((2 if roomy else 1, ff, width), BF16),
        pltpu.VMEM((local, nv, ff, span), BF16),
        pltpu.VMEM(tok.shape, BF16),
        pltpu.VMEM(lead.shape, BF16),
        pltpu.VMEM(heat.shape, jnp.int32),
        pltpu.VMEM(choice.shape, jnp.int32),
        pltpu.VMEM(router.shape, BF16),
        pltpu.VMEM((side, side), F32),
        pltpu.VMEM((groups, n, UNIT, wide), BF16),
        pltpu.VMEM((tokens, width), BF16),
        pltpu.VMEM((tokens, 128), F32),
        pltpu.VMEM((local, tokens, ff), BF16),
        pltpu.VMEM((depth, tile, tokens), F32),
        pltpu.VMEM((nq, nx, ne, per, span), link),
        pltpu.VMEM((nq, nx, ne, per, span), link),
        pltpu.VMEM((nq, nx, ne, per, span), link),
        pltpu.VMEM((nq, n3 - 1, n1 * n2, per, span) if roomy else (8, 128), BF16),
        pltpu.VMEM((nq, n3 - 1, n1 * n2, per, span), BF16),
        pltpu.VMEM((nq, n2 - 1, n1, per, span), BF16),
        pltpu.VMEM((nq, n2 - 1, n1, per, span), BF16),
        pltpu.VMEM((nq, n1 - 1, per, span), BF16),
        pltpu.VMEM((nq, n1 - 1, per, span), BF16),
        pltpu.VMEM((nq, n1, per, span), F32),
        pltpu.VMEM((2, tokens), F32),
        pltpu.VMEM((n, 2, tokens), F32),
        dma((6,)),
        dma((tiles,)),
        dma((2, local)),
        dma((local,)),
        dma((groups, n - 1)),
        dma((groups, n)),
        dma((nq, nx)),
        dma((nq, nx)),
        dma((nq, n3 - 1, n1 * n2)),
        dma((nq, n3 - 1, n1 * n2)),
        dma((nq, n2 - 1, n1)),
        dma((nq, n2 - 1, n1)),
        dma((nq, n1 - 1)),
        dma((nq, n1 - 1)),
        dma((n,)),
        dma((n,)),
    ]
    return pl.pallas_call(
        functools.partial(body, dims),
        out_shape=(
            jax.ShapeDtypeStruct((tiles * tile, tokens), F32),
            jax.ShapeDtypeStruct((1, tokens), F32),
            jax.ShapeDtypeStruct((rows, span), BF16),
        ),
        in_specs=[ANY] * 9,
        out_specs=(ANY, VMEM, VMEM),
        scratch_shapes=scratch,
        compiler_params=pltpu.CompilerParams(
            collective_id=0, has_side_effects=True, vmem_limit_bytes=67043328
        ),
        name="fused",
    )(lead, heat, embed, tok, choice, router, wg, wu, wd)


def per_device(dims, lead, heat, embed, tok, choice, router, wg, wu, wd):
    scaled, norm, moe = fused(
        dims,
        lead,
        heat[None, :],
        embed,
        tok.reshape(tok.shape[0] // UNIT, UNIT, tok.shape[1]),
        choice.T,
        router.T,
        wg.swapaxes(1, 2),
        wu.swapaxes(1, 2),
        wd,
    )
    return (scaled[: embed.shape[0]] - norm).T, moe


def fast_steps(mesh, axis):
    index = mesh.axis_names.index(axis)
    devices = mesh.devices.swapaxes(0, index)[:, 0]
    places = [tuple(d.coords) for d in devices]
    moved = [i for i, (p, q) in enumerate(zip(places[0], places[1])) if p != q]
    count = 1
    while count < len(places):
        if any(p != q and i not in moved for i, (p, q) in enumerate(zip(places[0], places[count]))):
            break
        count += 1
    return count


def solution(mesh):
    nv, ne = mesh.shape["vocab"], mesh.shape["expert"]
    nb = fast_steps(mesh, "expert")
    dims = (nv, ne, nv // CORES, ne // nb, nb)
    placed = (
        P(("vocab", "expert"), None),
        P(),
        P(("vocab", "expert"), None),
        P("expert", None),
        P("expert", None),
        P(),
        P("expert", None, "vocab"),
        P("expert", None, "vocab"),
        P("expert", "vocab", None),
    )
    return jax.shard_map(
        functools.partial(per_device, dims),
        mesh=mesh,
        in_specs=placed,
        out_specs=(P(None, ("vocab", "expert")), P("expert", "vocab")),
        check_vma=False,
    )
```

```python
import functools

import jax
import jax.numpy as jnp
from jax import lax
from jax.experimental import pallas as pl
from jax.experimental.pallas import tpu as pltpu
from jax.sharding import PartitionSpec as P

MESH = pl.DeviceIdType.MESH
ANY = pl.BlockSpec(memory_space=pl.ANY)
VMEM = pl.BlockSpec(memory_space=pltpu.VMEM)
CORES = 2
UNIT = 8
F32 = jnp.float32
BF16 = jnp.bfloat16


def dot_nt(a, b):
    return lax.dot_general(a, b, (((1,), (1,)), ((), ())), preferred_element_type=F32)


def body(
    dims,
    lead_ref, heat_ref, embed_ref, tok_ref, choice_ref, router_ref, wg_ref, wu_ref, wd_ref,
    sc_ref, norm_ref, moe_ref,
    embed_v, wg_v, wu_v, wd_raw, wd_v, xblk, lead_v, heat_v, choice_v, router_v, ptile, held, x2, pcol,
    act, logits, s_send, s_own, s_recv, sb3, rb3, sb2, rb2, sbz, rbz, acc, stat_mine, stat_all,
    sem_small, sem_l, sem_w, sem_raw, gs, gr, sem_ss, sem_sr, s3s, s3r, s2s, s2r, szs, szr, st_s, st_r,
):
    nv, ne, nx, na, nb = dims
    n = nv * ne
    v = lax.axis_index("vocab")
    e = lax.axis_index("expert")
    x, c = v // CORES, lax.rem(v, CORES)
    a, b = e // nb, lax.rem(e, nb)
    n1, n2, n3 = na, nb, nx
    if nx == nb:
        p2 = jnp.where(c == 0, b, x)
        p3 = jnp.where(c == 0, x, b)
    else:
        p2, p3 = b, x

    def dev(a_, p2_, p3_, c_):
        if nx == nb:
            b_ = jnp.where(c == 0, p2_, p3_)
            x_ = jnp.where(c == 0, p3_, p2_)
        else:
            b_, x_ = p2_, p3_
        return (x_ * CORES + c_, a_ * nb + b_)

    def wrap(i, size):
        return jnp.where(i >= size, i - size, i)

    groups = held.shape[0]
    nq = groups - 1

    def near(da, d2, d3):
        return wrap(a + da, n1), wrap(p2 + d2, n2), wrap(p3 + d3, n3)

    def slot(g, a_, p2_, p3_, c_):
        v_, e_ = dev(a_, p2_, p3_, c_)
        return v_ * ne + e_ if g == nq else e_ * nv + v_

    me = e * nv + v
    width = xblk.shape[2]
    nexp = router_v.shape[0]
    local, ff, _ = wg_v.shape
    raw_depth = wd_raw.shape[0]
    span = wd_v.shape[3]
    rows = xblk.shape[0] * UNIT

    small = [
        pltpu.make_async_copy(tok_ref, xblk, sem_small.at[0]),
        pltpu.make_async_copy(choice_ref, choice_v, sem_small.at[1]),
        pltpu.make_async_copy(router_ref, router_v, sem_small.at[2]),
        pltpu.make_async_copy(heat_ref, heat_v, sem_small.at[3]),
        pltpu.make_async_copy(lead_ref, lead_v, sem_small.at[4]),
    ]
    raw = [pltpu.make_async_copy(wd_ref.at[l], wd_raw.at[l % raw_depth], sem_raw.at[l]) for l in range(local)]
    wg_in = [pltpu.make_async_copy(wg_ref.at[l], wg_v.at[l], sem_w.at[0, l]) for l in range(local)]
    wu_in = [pltpu.make_async_copy(wu_ref.at[l], wu_v.at[l], sem_w.at[1, l]) for l in range(local)]
    depth, tile = logits.shape[0], logits.shape[1]
    vocab = embed_ref.shape[0]
    tiles = -(-vocab // tile)

    def extent(t):
        return t * tile, min(tile, vocab - t * tile)

    def sc_out(t):
        at = t * tile
        return pltpu.make_async_copy(
            logits.at[t % depth], sc_ref.at[at : at + tile], sem_l.at[t]
        )

    embed_in = pltpu.make_async_copy(embed_ref, embed_v, sem_small.at[5])

    for copy in small:
        copy.start()

    barrier = pltpu.get_barrier_semaphore()

    peers = [[dev(*near(d, 0, 0), c) for d in range(1, n1)]]
    peers += [
        [
            dev(*near(0, d2, d3), c if dc == 0 else 1 - c)
            for dc in range(CORES)
            for d3 in range(n3)
            for d2 in range(n2)
            if dc or d3 or d2
        ]
    ]
    for target in sum(peers, []):
        pl.semaphore_signal(barrier, inc=1, device_id=target, device_id_type=MESH)

    for l in range(min(raw_depth, local)):
        raw[l].start()

    for copy in small:
        copy.wait()
    scores = dot_nt(router_v[...], xblk[...].reshape(rows, width))
    ids = choice_v[...]
    expert = lax.broadcasted_iota(jnp.int32, (nexp, rows), 0)
    hot = expert == ids[0:1, :]
    for k in range(1, ids.shape[0]):
        hot = jnp.logical_or(hot, expert == ids[k : k + 1, :])
    peak = jnp.max(jnp.where(hot, scores, -jnp.inf), axis=0, keepdims=True)
    weight = jnp.where(hot, jnp.exp(jnp.where(hot, scores - peak, 0.0)), 0.0)
    prob = weight / jnp.sum(weight, axis=0, keepdims=True)
    high = prob.astype(BF16).astype(F32)
    ptile[...] = jnp.zeros_like(ptile)
    ptile[0:nexp, 0:rows] = high
    ptile[nexp : 2 * nexp, 0:rows] = prob - high
    ptile[...] = ptile[...].T
    for q in range(nq):
        unit = v * nq + q
        held[q, me, :, 0:width] = xblk[unit]
        start = pl.multiple_of(unit * UNIT, UNIT)
        held[q, me, :, width : width + 2 * nexp] = ptile[pl.ds(start, UNIT), 0 : 2 * nexp].astype(
            BF16
        )

    held[nq, v * ne + e, :, 0:width] = lead_v[...]

    pl.semaphore_wait(barrier, len(sum(peers, [])))

    base2 = n1 - 1
    base3 = base2 + (n2 - 1) * n1
    base_s = base3 + (n3 - 1) * n1 * n2

    def gcopy(g, s, k, target):
        return pltpu.make_async_remote_copy(
            src_ref=held.at[g, s],
            dst_ref=held.at[g, s],
            send_sem=gs.at[g, k],
            recv_sem=gr.at[g, s],
            device_id=target,
            device_id_type=MESH,
        )

    def forward(g, da, d2, d3, stage):
        s = slot(g, *near(da, d2, d3), c)
        if stage <= 1:
            for k2 in range(1, n2):
                gcopy(g, s, base2 + (k2 - 1) * n1 + da, dev(*near(0, k2, 0), c)).start()
        if stage <= 2:
            for k3 in range(1, n3):
                gcopy(g, s, base3 + ((k3 - 1) * n2 + d2) * n1 + da, dev(*near(0, 0, k3), c)).start()
        gcopy(g, s, base_s + (d3 * n2 + d2) * n1 + da, dev(a, p2, p3, 1 - c)).start()

    def arrive(g, s):
        gcopy(g, s, 0, dev(a, p2, p3, 1 - c)).wait_recv()

    def g_start(g):
        for d in range(1, n1):
            gcopy(g, slot(g, a, p2, p3, c), d - 1, dev(*near(d, 0, 0), c)).start()

    def g_own(g):
        forward(g, 0, 0, 0, 1)

    def g_one(g):
        @pl.loop(1, n1)
        def _(da):
            arrive(g, slot(g, *near(da, 0, 0), c))
            forward(g, da, 0, 0, 1)

    def g_two(g):
        for d2 in range(1, n2):

            @pl.loop(0, n1)
            def _(da):
                arrive(g, slot(g, *near(da, d2, 0), c))
                forward(g, da, d2, 0, 2)

    def g_three(g, d2s=None):
        for d2 in range(n2) if d2s is None else d2s:
            for d3 in range(1, n3):

                @pl.loop(0, n1)
                def _(da):
                    arrive(g, slot(g, *near(da, d2, d3), c))
                    forward(g, da, d2, d3, 3)

    def g_sib(g):
        for d3 in range(n3):
            for d2 in range(n2):

                @pl.loop(0, n1)
                def _(da):
                    arrive(g, slot(g, *near(da, d2, d3), 1 - c))

    def g_end(g):
        @pl.loop(0, n - 1)
        def _(k):
            gcopy(g, me, k, dev(a, p2, p3, 1 - c)).wait_send()

    def wd_shift(l):
        raw[l].wait()
        for w in range(nv):
            wd_v[l, w] = wd_raw[l % raw_depth, :, w * span : (w + 1) * span]
        if l + raw_depth < local:
            raw[l + raw_depth].start()

    def load_x(g):
        x2[...] = held[g, :, :, 0:width].reshape(n * UNIT, width)

    def load_p(q):
        tail = held[q, :, :, width : width + 2 * nexp].reshape(n * UNIT, 2 * nexp).astype(F32)
        lane = lax.rem(lax.broadcasted_iota(jnp.int32, tail.shape, 1), nexp)
        for l in range(local):
            pcol[:, l : l + 1] = jnp.sum(
                jnp.where(lane == e * local + l, tail, 0.0), axis=1, keepdims=True
            )

    def gate_up(l):
        gate = dot_nt(wg_v[l], x2[...])
        up = dot_nt(wu_v[l], x2[...])
        act[l] = (gate * jax.nn.sigmoid(1.702 * gate) * (up + 1.0)).astype(BF16).T

    def down(w):
        total = pcol[:, 0:1] * jnp.dot(act[0], wd_v[0, w], preferred_element_type=F32)
        for l in range(1, local):
            total += pcol[:, l : l + 1] * jnp.dot(act[l], wd_v[l, w], preferred_element_type=F32)
        return total.reshape(ne, n * UNIT // ne, span)

    def scopy(q, j):
        return pltpu.make_async_remote_copy(
            src_ref=s_send.at[q, j],
            dst_ref=s_recv.at[q, j],
            send_sem=sem_ss.at[q, j],
            recv_sem=sem_sr.at[q, j],
            device_id=dev(a, p2, p3, 1 - c),
            device_id_type=MESH,
        )

    def down_send(q, dx):
        j = wrap(x + dx, nx)
        s_send[q, j] = down(j * CORES + 1 - c).astype(s_send.dtype)
        scopy(q, j).start()

    def down_own(q, dx):
        j = wrap(x + dx, nx)
        s_own[q, j] = down(j * CORES + c).astype(s_own.dtype)

    def chip(q, a_, p2_, p3_):
        v_, e_ = dev(a_, p2_, p3_, c)
        x_ = v_ // CORES
        return s_own[q, x_, e_].astype(F32) + s_recv[q, x_, e_].astype(F32)

    shared = len(sb3.shape) == 2
    sb3 = s_send if shared else sb3

    def c3(q, d3, i, target):
        return pltpu.make_async_remote_copy(
            src_ref=sb3.at[q, d3 - 1, i],
            dst_ref=rb3.at[q, d3 - 1, i],
            send_sem=s3s.at[q, d3 - 1, i],
            recv_sem=s3r.at[q, d3 - 1, i],
            device_id=target,
            device_id_type=MESH,
        )

    def c2(q, d2, i, target):
        return pltpu.make_async_remote_copy(
            src_ref=sb2.at[q, d2 - 1, i],
            dst_ref=rb2.at[q, d2 - 1, i],
            send_sem=s2s.at[q, d2 - 1, i],
            recv_sem=s2r.at[q, d2 - 1, i],
            device_id=target,
            device_id_type=MESH,
        )

    def c1(q, d, target):
        return pltpu.make_async_remote_copy(
            src_ref=sbz.at[q, d - 1],
            dst_ref=rbz.at[q, d - 1],
            send_sem=szs.at[q, d - 1],
            recv_sem=szr.at[q, d - 1],
            device_id=target,
            device_id_type=MESH,
        )

    def c_unit(q, da, d2, d3):
        a_, p2_, p3_ = near(da, d2, d3)
        k = a_ * n2 + p2_
        sb3[q, d3 - 1, k] = chip(q, a_, p2_, p3_).astype(BF16)
        c3(q, d3, k, dev(*near(0, 0, d3), c)).start()

    def c_send(q, dx):
        def lead_x():
            for d2 in range(n2 - 1, -1, -1):
                pl.loop(0, n1)(lambda i: c_unit(q, wrap(i + 1, n1), d2, dx))

        def lead_b():
            for d3 in range(1, n3):
                pl.loop(0, n1)(lambda i: c_unit(q, wrap(i + 1, n1), dx, d3))

        scopy(q, wrap(x + dx, nx)).wait_recv()
        if nx == nb:
            if dx:
                pl.when(c == 0)(lead_x)
            pl.when(c == 1)(lead_b)
        elif dx:
            lead_x()

    def down_all(q, extra):
        order = list(range(1, nx)) + [0]
        for dx in order:
            down_send(q, dx)
            if extra:
                extra.pop(0)()
        if shared:
            for dx in order:
                scopy(q, wrap(x + dx, nx)).wait_send()
        for dx in order:
            down_own(q, dx)
            c_send(q, dx)
            if extra:
                extra.pop(0)()
        for step in extra:
            step()

    def c_three(q, own):
        def total(da, d2):
            a_, p2_, p3_ = near(da, d2, 0)
            k = a_ * n2 + p2_
            part = chip(q, a_, p2_, p3_)
            for d3 in range(1, n3):
                c3(q, d3, k, dev(a, p2, p3, 1 - c)).wait_recv()
                part += rb3[q, d3 - 1, k].astype(F32)
            return a_, part

        for d2 in range(0 if own else n2 - 1, 0, -1):

            @pl.loop(0, n1)
            def _(i):
                a_, part = total(wrap(i + 1, n1), d2)
                sb2[q, d2 - 1, a_] = part.astype(BF16)
                c2(q, d2, a_, dev(*near(0, d2, 0), c)).start()

        if own:

            @pl.loop(0, n1)
            def _(i):
                a_, part = total(wrap(i + 1, n1), 0)
                acc[q, a_] = part

    def c_two(q):
        def total(a_):
            part = acc[q, a_]
            for d2 in range(1, n2):
                c2(q, d2, a_, dev(a, p2, p3, 1 - c)).wait_recv()
                part += rb2[q, d2 - 1, a_].astype(F32)
            return part

        @pl.loop(1, n1)
        def _(da):
            a_, p2_, p3_ = near(da, 0, 0)
            sbz[q, da - 1] = total(a_).astype(BF16)
            c1(q, da, dev(a_, p2_, p3_, c)).start()

        acc[q, a] = total(a)

    def c_one(q):
        part = acc[q, a]
        for d in range(1, n1):
            c1(q, d, dev(a, p2, p3, 1 - c)).wait_recv()
            part += rbz[q, d - 1].astype(F32)
        part = part.astype(BF16)
        for w in range(nv):
            at = (w * nq + q) * UNIT
            moe_ref[at : at + UNIT, :] = part[w * UNIT : (w + 1) * UNIT]

    def c_end(q):
        nobody = dev(a, p2, p3, 1 - c)

        if not shared:

            @pl.loop(0, nx)
            def _(j):
                scopy(q, j).wait_send()

        for d3 in range(1, n3):

            @pl.loop(0, n1 * n2)
            def _(i):
                c3(q, d3, i, nobody).wait_send()

        for d2 in range(1, n2):

            @pl.loop(0, n1)
            def _(i):
                c2(q, d2, i, nobody).wait_send()

        for d in range(1, n1):
            c1(q, d, nobody).wait_send()

    def lm_tile(t, top, total):
        at, size = extent(t)
        if t == 0:
            embed_in.wait()
        scale = 1.0 / (0.5 + 0.25 * heat_v[...].astype(F32))
        part = dot_nt(embed_v[at : at + size], x2[...]) * scale
        if t >= depth:
            sc_out(t - depth).wait()
        logits[t % depth, 0:size] = part
        sc_out(t).start()
        peak = jnp.maximum(top, jnp.max(part, axis=0, keepdims=True))
        total = total * jnp.exp(top - peak) + jnp.sum(jnp.exp(part - peak), axis=0, keepdims=True)
        return peak, total

    def stat(stage, d):
        k = sum(len(p) for p in peers[:stage]) + d
        return pltpu.make_async_remote_copy(
            src_ref=stat_mine.at[stage],
            dst_ref=stat_all.at[k],
            send_sem=st_s.at[k],
            recv_sem=st_r.at[k],
            device_id=peers[stage][d],
            device_id_type=MESH,
        )

    def stat_send(stage, top, total):
        stat_mine[stage, 0:1, :] = top
        stat_mine[stage, 1:2, :] = total
        for d in range(len(peers[stage])):
            stat(stage, d).start()

    def stat_merge(stage):
        top, total = stat_mine[stage, 0:1, :], stat_mine[stage, 1:2, :]
        for d in range(len(peers[stage])):
            stat(stage, d).wait()
            k = sum(len(p) for p in peers[:stage]) + d
            peak = jnp.maximum(top, stat_all[k, 0:1, :])
            total = total * jnp.exp(top - peak) + stat_all[k, 1:2, :] * jnp.exp(
                stat_all[k, 0:1, :] - peak
            )
            top = peak
        if stage + 1 < len(peers):
            stat_send(stage + 1, top, total)
        else:
            norm_ref[...] = top + jnp.log(total)

    last = nq
    g_start(0)
    g_own(0)
    for l in range(local - 2):
        wd_shift(l)
    for l in range(local):
        wg_in[l].start()
        wu_in[l].start()
    embed_in.start()
    g_one(0)
    for g in range(1, nq):
        g_start(g)
    wd_shift(local - 2)
    g_two(0)
    for g in range(1, nq):
        g_own(g)
        g_one(g)
    g_start(last)
    wd_shift(local - 1)
    g_three(0)
    g_own(last)
    g_sib(0)
    load_x(0)
    load_p(0)

    def during(q):
        steps = [[] for _ in range(local)]
        tail = []

        def put(at, *fs):
            steps[min(at, local - 1)].extend(fs)

        if q + 1 < nq:
            put(0, lambda: g_two(q + 1))
            put(2, lambda: g_three(q + 1, [0]))
            put(3, lambda: g_three(q + 1, range(1, n2)))
        if q == 0:
            put(1, lambda: g_one(last))
            tail += [lambda: None, lambda: g_two(last)]
        if q == nq - 1:
            put(1, lambda: g_three(last, [0]))
            put(local, lambda: g_three(last, range(1, n2)))
        if q:
            put(2, lambda: c_three(q - 1, False))
            put(local, lambda: c_three(q - 1, True))
            tail += [lambda: None, lambda: c_two(q - 1)]
        return steps, tail

    for q in range(nq):
        if q:
            g_sib(q)
            load_x(q)
            load_p(q)
        steps, tail = during(q)
        for l in range(local):
            if q == 0:
                wg_in[l].wait()
                wu_in[l].wait()
            gate_up(l)
            for extra in steps[l]:
                extra()
        down_all(q, tail)
    q = nq - 1
    g_sib(last)
    load_x(last)
    steps = {tiles // 2: lambda: c_three(q, False)}
    top, total = jnp.full((1, n * UNIT), -jnp.inf, F32), jnp.zeros((1, n * UNIT), F32)
    for t in range(tiles):
        if t in steps:
            steps[t]()
        top, total = lm_tile(t, top, total)
    stat_send(0, top, total)
    c_three(q, True)
    c_two(q)
    for k in range(q):
        c_one(k)
    for g in range(groups):
        g_end(g)
    stat_merge(0)
    c_one(q)
    for k in range(nq):
        c_end(k)
    stat_merge(1)
    for t in range(max(0, tiles - depth), tiles):
        sc_out(t).wait()


def fused(dims, lead, heat, embed, tok, choice, router, wg, wu, wd):
    nv, ne, nx, na, nb = dims
    n = nv * ne
    local, ff, width = wg.shape
    vocab = embed.shape[0]
    rows = tok.shape[0] * UNIT
    nexp = router.shape[0]
    span = width // nv
    nq = tok.shape[0] // nv
    groups = nq + 1
    tokens = n * UNIT
    wide = -(-(width + 2 * nexp) // 128) * 128
    per = tokens // ne
    side = -(-max(2 * nexp, rows) // 128) * 128
    n1, n2, n3 = na, nb, nx
    roomy = 3 * nx * nq * tokens * (-(-span // 128) * 128) * 4 < 10 << 20
    tile = -(-vocab // (32 if roomy else 128)) * 16
    tiles = -(-vocab // tile)
    link, depth = (F32, tiles) if roomy else (BF16, 2)
    n_peers = n1 - 1 + n2 * n3 * CORES - 1
    dma = pltpu.SemaphoreType.DMA
    scratch = [
        pltpu.VMEM((vocab, width), BF16),
        pltpu.VMEM((local, ff, width), BF16),
        pltpu.VMEM((local, ff, width), BF16),
        pltpu.VMEM((2 if roomy else 1, ff, width), BF16),
        pltpu.VMEM((local, nv, ff, span), BF16),
        pltpu.VMEM(tok.shape, BF16),
        pltpu.VMEM(lead.shape, BF16),
        pltpu.VMEM(heat.shape, jnp.int32),
        pltpu.VMEM(choice.shape, jnp.int32),
        pltpu.VMEM(router.shape, BF16),
        pltpu.VMEM((side, side), F32),
        pltpu.VMEM((groups, n, UNIT, wide), BF16),
        pltpu.VMEM((tokens, width), BF16),
        pltpu.VMEM((tokens, 128), F32),
        pltpu.VMEM((local, tokens, ff), BF16),
        pltpu.VMEM((depth, tile, tokens), F32),
        pltpu.VMEM((nq, nx, ne, per, span), link),
        pltpu.VMEM((nq, nx, ne, per, span), link),
        pltpu.VMEM((nq, nx, ne, per, span), link),
        pltpu.VMEM((nq, n3 - 1, n1 * n2, per, span) if roomy else (8, 128), BF16),
        pltpu.VMEM((nq, n3 - 1, n1 * n2, per, span), BF16),
        pltpu.VMEM((nq, n2 - 1, n1, per, span), BF16),
        pltpu.VMEM((nq, n2 - 1, n1, per, span), BF16),
        pltpu.VMEM((nq, n1 - 1, per, span), BF16),
        pltpu.VMEM((nq, n1 - 1, per, span), BF16),
        pltpu.VMEM((nq, n1, per, span), F32),
        pltpu.VMEM((2, 2, tokens), F32),
        pltpu.VMEM((n_peers, 2, tokens), F32),
        dma((6,)),
        dma((tiles,)),
        dma((2, local)),
        dma((local,)),
        dma((groups, n - 1)),
        dma((groups, n)),
        dma((nq, nx)),
        dma((nq, nx)),
        dma((nq, n3 - 1, n1 * n2)),
        dma((nq, n3 - 1, n1 * n2)),
        dma((nq, n2 - 1, n1)),
        dma((nq, n2 - 1, n1)),
        dma((nq, n1 - 1)),
        dma((nq, n1 - 1)),
        dma((n_peers,)),
        dma((n_peers,)),
    ]
    return pl.pallas_call(
        functools.partial(body, dims),
        out_shape=(
            jax.ShapeDtypeStruct((tiles * tile, tokens), F32),
            jax.ShapeDtypeStruct((1, tokens), F32),
            jax.ShapeDtypeStruct((rows, span), BF16),
        ),
        in_specs=[ANY] * 9,
        out_specs=(ANY, VMEM, VMEM),
        scratch_shapes=scratch,
        compiler_params=pltpu.CompilerParams(
            collective_id=0, has_side_effects=True, vmem_limit_bytes=67043328
        ),
        name="fused",
    )(lead, heat, embed, tok, choice, router, wg, wu, wd)


def per_device(dims, lead, heat, embed, tok, choice, router, wg, wu, wd):
    scaled, norm, moe = fused(
        dims,
        lead,
        heat[None, :],
        embed,
        tok.reshape(tok.shape[0] // UNIT, UNIT, tok.shape[1]),
        choice.T,
        router.T,
        wg.swapaxes(1, 2),
        wu.swapaxes(1, 2),
        wd,
    )
    return (scaled[: embed.shape[0]] - norm).T, moe


def fast_steps(mesh, axis):
    index = mesh.axis_names.index(axis)
    devices = mesh.devices.swapaxes(0, index)[:, 0]
    places = [tuple(d.coords) for d in devices]
    moved = [i for i, (p, q) in enumerate(zip(places[0], places[1])) if p != q]
    count = 1
    while count < len(places):
        if any(p != q and i not in moved for i, (p, q) in enumerate(zip(places[0], places[count]))):
            break
        count += 1
    return count


def solution(mesh):
    nv, ne = mesh.shape["vocab"], mesh.shape["expert"]
    nb = fast_steps(mesh, "expert")
    dims = (nv, ne, nv // CORES, ne // nb, nb)
    placed = (
        P(("vocab", "expert"), None),
        P(),
        P(("vocab", "expert"), None),
        P("expert", None),
        P("expert", None),
        P(),
        P("expert", None, "vocab"),
        P("expert", None, "vocab"),
        P("expert", "vocab", None),
    )
    return jax.shard_map(
        functools.partial(per_device, dims),
        mesh=mesh,
        in_specs=placed,
        out_specs=(P(None, ("vocab", "expert")), P("expert", "vocab")),
        check_vma=False,
    )
```

```python
import functools

import jax
import jax.numpy as jnp
from jax import lax
from jax.experimental import pallas as pl
from jax.experimental.pallas import tpu as pltpu
from jax.sharding import PartitionSpec as P

MESH = pl.DeviceIdType.MESH
ANY = pl.BlockSpec(memory_space=pl.ANY)
VMEM = pl.BlockSpec(memory_space=pltpu.VMEM)
CORES = 2
UNIT = 8
F32 = jnp.float32
BF16 = jnp.bfloat16


def dot_nt(a, b):
    return lax.dot_general(a, b, (((1,), (1,)), ((), ())), preferred_element_type=F32)


def body(
    dims,
    lead_ref, heat_ref, embed_ref, tok_ref, choice_ref, router_ref, wg_ref, wu_ref, wd_ref,
    sc_ref, norm_ref, moe_ref,
    embed_v, wg_v, wu_v, wd_raw, wd_v, xblk, lead_v, heat_v, choice_v, router_v, ptile, held, x2, pcol,
    act, logits, s_send, s_own, s_recv, sb3, rb3, sb2, rb2, sbz, rbz, acc, stat_mine, stat_all,
    sem_small, sem_l, sem_w, sem_raw, gs, gr, sem_ss, sem_sr, s3s, s3r, s2s, s2r, szs, szr, st_s, st_r,
):
    nv, ne, nx, na, nb = dims
    n = nv * ne
    v = lax.axis_index("vocab")
    e = lax.axis_index("expert")
    x, c = v // CORES, lax.rem(v, CORES)
    a, b = e // nb, lax.rem(e, nb)
    n1, n2, n3 = na, nb, nx
    if nx == nb:
        p2 = jnp.where(c == 0, b, x)
        p3 = jnp.where(c == 0, x, b)
    else:
        p2, p3 = b, x

    def dev(a_, p2_, p3_, c_):
        if nx == nb:
            b_ = jnp.where(c == 0, p2_, p3_)
            x_ = jnp.where(c == 0, p3_, p2_)
        else:
            b_, x_ = p2_, p3_
        return (x_ * CORES + c_, a_ * nb + b_)

    def wrap(i, size):
        return jnp.where(i >= size, i - size, i)

    groups = held.shape[0]
    nq = groups - 1

    def near(da, d2, d3):
        return wrap(a + da, n1), wrap(p2 + d2, n2), wrap(p3 + d3, n3)

    def slot(g, a_, p2_, p3_, c_):
        v_, e_ = dev(a_, p2_, p3_, c_)
        return v_ * ne + e_ if g == nq else e_ * nv + v_

    me = e * nv + v
    width = xblk.shape[2]
    nexp = router_v.shape[0]
    local, ff, _ = wg_v.shape
    raw_depth = wd_raw.shape[0]
    span = wd_v.shape[3]
    rows = xblk.shape[0] * UNIT

    small = [
        pltpu.make_async_copy(tok_ref, xblk, sem_small.at[0]),
        pltpu.make_async_copy(choice_ref, choice_v, sem_small.at[1]),
        pltpu.make_async_copy(router_ref, router_v, sem_small.at[2]),
        pltpu.make_async_copy(heat_ref, heat_v, sem_small.at[3]),
        pltpu.make_async_copy(lead_ref, lead_v, sem_small.at[4]),
    ]
    raw = [pltpu.make_async_copy(wd_ref.at[l], wd_raw.at[l % raw_depth], sem_raw.at[l]) for l in range(local)]
    wg_in = [pltpu.make_async_copy(wg_ref.at[l], wg_v.at[l], sem_w.at[0, l]) for l in range(local)]
    wu_in = [pltpu.make_async_copy(wu_ref.at[l], wu_v.at[l], sem_w.at[1, l]) for l in range(local)]
    depth, tile = logits.shape[0], logits.shape[1]
    vocab = embed_ref.shape[0]
    streamed = tile < vocab
    tile = tile if streamed else vocab
    tiles = -(-vocab // tile)

    def extent(t):
        return t * tile, min(tile, vocab - t * tile)

    def sc_out(t):
        at = t * tile
        return pltpu.make_async_copy(
            logits.at[t % depth], sc_ref.at[at : at + tile], sem_l.at[t]
        )

    embed_in = pltpu.make_async_copy(embed_ref, embed_v, sem_small.at[5])

    for copy in small:
        copy.start()

    barrier = pltpu.get_barrier_semaphore()

    peers = [[dev(*near(d, 0, 0), c) for d in range(1, n1)]]
    peers += [
        [
            dev(*near(0, d2, d3), c if dc == 0 else 1 - c)
            for dc in range(CORES)
            for d3 in range(n3)
            for d2 in range(n2)
            if dc or d3 or d2
        ]
    ]
    for target in sum(peers, []):
        pl.semaphore_signal(barrier, inc=1, device_id=target, device_id_type=MESH)

    for l in range(min(raw_depth, local)):
        raw[l].start()

    for copy in small:
        copy.wait()
    scores = dot_nt(router_v[...], xblk[...].reshape(rows, width))
    ids = choice_v[...]
    expert = lax.broadcasted_iota(jnp.int32, (nexp, rows), 0)
    hot = expert == ids[0:1, :]
    for k in range(1, ids.shape[0]):
        hot = jnp.logical_or(hot, expert == ids[k : k + 1, :])
    peak = jnp.max(jnp.where(hot, scores, -jnp.inf), axis=0, keepdims=True)
    weight = jnp.where(hot, jnp.exp(jnp.where(hot, scores - peak, 0.0)), 0.0)
    prob = weight / jnp.sum(weight, axis=0, keepdims=True)
    high = prob.astype(BF16).astype(F32)
    ptile[...] = jnp.zeros_like(ptile)
    ptile[0:nexp, 0:rows] = high
    ptile[nexp : 2 * nexp, 0:rows] = prob - high
    ptile[...] = ptile[...].T
    for q in range(nq):
        unit = v * nq + q
        held[q, me, :, 0:width] = xblk[unit]
        start = pl.multiple_of(unit * UNIT, UNIT)
        held[q, me, :, width : width + 2 * nexp] = ptile[pl.ds(start, UNIT), 0 : 2 * nexp].astype(
            BF16
        )

    held[nq, v * ne + e, :, 0:width] = lead_v[...]

    pl.semaphore_wait(barrier, len(sum(peers, [])))

    base2 = n1 - 1
    base3 = base2 + (n2 - 1) * n1
    base_s = base3 + (n3 - 1) * n1 * n2

    def gcopy(g, s, k, target):
        return pltpu.make_async_remote_copy(
            src_ref=held.at[g, s],
            dst_ref=held.at[g, s],
            send_sem=gs.at[g, k],
            recv_sem=gr.at[g, s],
            device_id=target,
            device_id_type=MESH,
        )

    def far(i):
        return jnp.where(2 * a < n1, n1 - i, i)

    def close(i):
        return jnp.where(i == 0, 0, jnp.where(2 * a < n1, i, n1 - i))

    def forward(g, da, d2, d3, stage):
        s = slot(g, *near(da, d2, d3), c)
        if stage <= 1:
            for k2 in range(1, n2):
                gcopy(g, s, base2 + (k2 - 1) * n1 + da, dev(*near(0, k2, 0), c)).start()
        if stage <= 2:
            for k3 in range(1, n3):
                gcopy(g, s, base3 + ((k3 - 1) * n2 + d2) * n1 + da, dev(*near(0, 0, k3), c)).start()
        gcopy(g, s, base_s + (d3 * n2 + d2) * n1 + da, dev(a, p2, p3, 1 - c)).start()

    def arrive(g, s):
        gcopy(g, s, 0, dev(a, p2, p3, 1 - c)).wait_recv()

    def g_start(g):
        for i in range(1, n1):
            d = far(i)
            gcopy(g, slot(g, a, p2, p3, c), d - 1, dev(*near(d, 0, 0), c)).start()

    def g_own(g):
        forward(g, 0, 0, 0, 1)

    def g_one(g):
        @pl.loop(1, n1)
        def _(i):
            da = close(i)
            arrive(g, slot(g, *near(da, 0, 0), c))
            forward(g, da, 0, 0, 1)

    def g_two(g):
        for d2 in range(1, n2):

            @pl.loop(0, n1)
            def _(i):
                da = close(i)
                arrive(g, slot(g, *near(da, d2, 0), c))
                forward(g, da, d2, 0, 2)

    def g_three(g, d2s=None):
        for d2 in range(n2) if d2s is None else d2s:
            for d3 in range(1, n3):

                @pl.loop(0, n1)
                def _(i):
                    da = close(i)
                    arrive(g, slot(g, *near(da, d2, d3), c))
                    forward(g, da, d2, d3, 3)

    def g_sib(g):
        for d3 in range(n3):
            for d2 in range(n2):

                @pl.loop(0, n1)
                def _(da):
                    arrive(g, slot(g, *near(da, d2, d3), 1 - c))

    def g_end(g):
        @pl.loop(0, n - 1)
        def _(k):
            gcopy(g, me, k, dev(a, p2, p3, 1 - c)).wait_send()

    def wd_shift(l):
        raw[l].wait()
        for w in range(nv):
            wd_v[l, w] = wd_raw[l % raw_depth, :, w * span : (w + 1) * span]
        if l + raw_depth < local:
            raw[l + raw_depth].start()

    def load_x(g):
        x2[...] = held[g, :, :, 0:width].reshape(n * UNIT, width)

    def load_p(q):
        tail = held[q, :, :, width : width + 2 * nexp].reshape(n * UNIT, 2 * nexp).astype(F32)
        lane = lax.rem(lax.broadcasted_iota(jnp.int32, tail.shape, 1), nexp)
        for l in range(local):
            pcol[:, l : l + 1] = jnp.sum(
                jnp.where(lane == e * local + l, tail, 0.0), axis=1, keepdims=True
            )

    def gate_up(l):
        gate = dot_nt(wg_v[l], x2[...])
        up = dot_nt(wu_v[l], x2[...])
        act[l] = (gate * jax.nn.sigmoid(1.702 * gate) * (up + 1.0)).astype(BF16).T

    def down(w):
        total = pcol[:, 0:1] * jnp.dot(act[0], wd_v[0, w], preferred_element_type=F32)
        for l in range(1, local):
            total += pcol[:, l : l + 1] * jnp.dot(act[l], wd_v[l, w], preferred_element_type=F32)
        return total.reshape(ne, n * UNIT // ne, span)

    def scopy(q, j):
        return pltpu.make_async_remote_copy(
            src_ref=s_send.at[q, j],
            dst_ref=s_recv.at[q, j],
            send_sem=sem_ss.at[q, j],
            recv_sem=sem_sr.at[q, j],
            device_id=dev(a, p2, p3, 1 - c),
            device_id_type=MESH,
        )

    def down_send(q, dx):
        j = wrap(x + dx, nx)
        s_send[q, j] = down(j * CORES + 1 - c).astype(s_send.dtype)
        scopy(q, j).start()

    def down_own(q, dx):
        j = wrap(x + dx, nx)
        s_own[q, j] = down(j * CORES + c).astype(s_own.dtype)

    def chip(q, a_, p2_, p3_):
        v_, e_ = dev(a_, p2_, p3_, c)
        x_ = v_ // CORES
        return s_own[q, x_, e_].astype(F32) + s_recv[q, x_, e_].astype(F32)

    shared = len(sb3.shape) == 2
    sb3 = s_send if shared else sb3

    def c3(q, d3, i, target):
        return pltpu.make_async_remote_copy(
            src_ref=sb3.at[q, d3 - 1, i],
            dst_ref=rb3.at[q, d3 - 1, i],
            send_sem=s3s.at[q, d3 - 1, i],
            recv_sem=s3r.at[q, d3 - 1, i],
            device_id=target,
            device_id_type=MESH,
        )

    def c2(q, d2, i, target):
        return pltpu.make_async_remote_copy(
            src_ref=sb2.at[q, d2 - 1, i],
            dst_ref=rb2.at[q, d2 - 1, i],
            send_sem=s2s.at[q, d2 - 1, i],
            recv_sem=s2r.at[q, d2 - 1, i],
            device_id=target,
            device_id_type=MESH,
        )

    def c1(q, d, target):
        return pltpu.make_async_remote_copy(
            src_ref=sbz.at[q, d - 1],
            dst_ref=rbz.at[q, d - 1],
            send_sem=szs.at[q, d - 1],
            recv_sem=szr.at[q, d - 1],
            device_id=target,
            device_id_type=MESH,
        )

    def c_unit(q, da, d2, d3):
        a_, p2_, p3_ = near(da, d2, d3)
        k = a_ * n2 + p2_
        sb3[q, d3 - 1, k] = chip(q, a_, p2_, p3_).astype(BF16)
        c3(q, d3, k, dev(*near(0, 0, d3), c)).start()

    def c_send(q, dx):
        def lead_x():
            for d2 in range(n2 - 1, -1, -1):
                pl.loop(0, n1)(lambda i: c_unit(q, wrap(i + 1, n1), d2, dx))

        def lead_b():
            for d3 in range(1, n3):
                pl.loop(0, n1)(lambda i: c_unit(q, wrap(i + 1, n1), dx, d3))

        scopy(q, wrap(x + dx, nx)).wait_recv()
        if nx == nb:
            if dx:
                pl.when(c == 0)(lead_x)
            pl.when(c == 1)(lead_b)
        elif dx:
            lead_x()

    def down_all(q, extra):
        order = list(range(1, nx)) + [0]
        for dx in order:
            down_send(q, dx)
            if extra:
                extra.pop(0)()
        if shared:
            for dx in order:
                scopy(q, wrap(x + dx, nx)).wait_send()
        for dx in order:
            down_own(q, dx)
            c_send(q, dx)
            if extra:
                extra.pop(0)()
        for step in extra:
            step()

    def c_three(q, own):
        def total(da, d2):
            a_, p2_, p3_ = near(da, d2, 0)
            k = a_ * n2 + p2_
            part = chip(q, a_, p2_, p3_)
            for d3 in range(1, n3):
                c3(q, d3, k, dev(a, p2, p3, 1 - c)).wait_recv()
                part += rb3[q, d3 - 1, k].astype(F32)
            return a_, part

        for d2 in range(0 if own else n2 - 1, 0, -1):

            @pl.loop(0, n1)
            def _(i):
                a_, part = total(wrap(i + 1, n1), d2)
                sb2[q, d2 - 1, a_] = part.astype(BF16)
                c2(q, d2, a_, dev(*near(0, d2, 0), c)).start()

        if own:

            @pl.loop(0, n1)
            def _(i):
                a_, part = total(wrap(i + 1, n1), 0)
                acc[q, a_] = part

    def c_two(q):
        def total(a_):
            part = acc[q, a_]
            for d2 in range(1, n2):
                c2(q, d2, a_, dev(a, p2, p3, 1 - c)).wait_recv()
                part += rb2[q, d2 - 1, a_].astype(F32)
            return part

        @pl.loop(1, n1)
        def _(i):
            da = far(i)
            a_, p2_, p3_ = near(da, 0, 0)
            sbz[q, da - 1] = total(a_).astype(BF16)
            c1(q, da, dev(a_, p2_, p3_, c)).start()

        acc[q, a] = total(a)

    def c_one(q):
        part = acc[q, a]
        for d in range(1, n1):
            c1(q, d, dev(a, p2, p3, 1 - c)).wait_recv()
            part += rbz[q, d - 1].astype(F32)
        part = part.astype(BF16)
        for w in range(nv):
            at = (w * nq + q) * UNIT
            moe_ref[at : at + UNIT, :] = part[w * UNIT : (w + 1) * UNIT]

    def c_end(q):
        nobody = dev(a, p2, p3, 1 - c)

        if not shared:

            @pl.loop(0, nx)
            def _(j):
                scopy(q, j).wait_send()

        for d3 in range(1, n3):

            @pl.loop(0, n1 * n2)
            def _(i):
                c3(q, d3, i, nobody).wait_send()

        for d2 in range(1, n2):

            @pl.loop(0, n1)
            def _(i):
                c2(q, d2, i, nobody).wait_send()

        for d in range(1, n1):
            c1(q, d, nobody).wait_send()

    def lm_tile(t, top, total):
        at, size = extent(t)
        if t == 0:
            embed_in.wait()
        scale = 1.0 / (0.5 + 0.25 * heat_v[...].astype(F32))
        part = dot_nt(embed_v[at : at + size], x2[...]) * scale
        if streamed:
            if t >= depth:
                sc_out(t - depth).wait()
            logits[t % depth, 0:size] = part
            sc_out(t).start()
        else:
            sc_ref[at : at + size] = part
        peak = jnp.maximum(top, jnp.max(part, axis=0, keepdims=True))
        total = total * jnp.exp(top - peak) + jnp.sum(jnp.exp(part - peak), axis=0, keepdims=True)
        return peak, total

    def stat(stage, d):
        k = sum(len(p) for p in peers[:stage]) + d
        return pltpu.make_async_remote_copy(
            src_ref=stat_mine.at[stage],
            dst_ref=stat_all.at[k],
            send_sem=st_s.at[k],
            recv_sem=st_r.at[k],
            device_id=peers[stage][d],
            device_id_type=MESH,
        )

    def stat_send(stage, top, total):
        stat_mine[stage, 0:1, :] = top
        stat_mine[stage, 1:2, :] = total
        for d in range(len(peers[stage])):
            stat(stage, d).start()

    def stat_merge(stage):
        top, total = stat_mine[stage, 0:1, :], stat_mine[stage, 1:2, :]
        for d in range(len(peers[stage])):
            stat(stage, d).wait()
            k = sum(len(p) for p in peers[:stage]) + d
            peak = jnp.maximum(top, stat_all[k, 0:1, :])
            total = total * jnp.exp(top - peak) + stat_all[k, 1:2, :] * jnp.exp(
                stat_all[k, 0:1, :] - peak
            )
            top = peak
        if stage + 1 < len(peers):
            stat_send(stage + 1, top, total)
        else:
            norm_ref[...] = top + jnp.log(total)

    last = nq
    g_start(0)
    g_own(0)
    for l in range(local - 2):
        wd_shift(l)
    for l in range(local):
        wg_in[l].start()
        wu_in[l].start()
    embed_in.start()
    g_one(0)
    for g in range(1, nq):
        g_start(g)
    wd_shift(local - 2)
    g_two(0)
    for g in range(1, nq):
        g_own(g)
        g_one(g)
    g_start(last)
    wd_shift(local - 1)
    g_three(0)
    g_own(last)
    g_sib(0)
    load_x(0)
    load_p(0)

    def during(q):
        steps = [[] for _ in range(local)]
        tail = []

        def put(at, *fs):
            steps[min(at, local - 1)].extend(fs)

        if q + 1 < nq:
            put(0, lambda: g_two(q + 1))
            put(2, lambda: g_three(q + 1, [0]))
            put(3, lambda: g_three(q + 1, range(1, n2)))
        if q == 0:
            put(1, lambda: g_one(last))
            tail += [lambda: None, lambda: g_two(last)]
        if q == nq - 1:
            put(1, lambda: g_three(last, [0]))
            put(local, lambda: g_three(last, range(1, n2)))
        if q:
            put(2, lambda: c_three(q - 1, False))
            put(local, lambda: c_three(q - 1, True))
            tail += [lambda: None, lambda: None, lambda: None, lambda: c_two(q - 1)]
        return steps, tail

    for q in range(nq):
        if q:
            g_sib(q)
            load_x(q)
            load_p(q)
        steps, tail = during(q)
        for l in range(local):
            if q == 0:
                wg_in[l].wait()
                wu_in[l].wait()
            gate_up(l)
            for extra in steps[l]:
                extra()
        down_all(q, tail)
    q = nq - 1
    g_sib(last)
    load_x(last)
    top, total = jnp.full((1, n * UNIT), -jnp.inf, F32), jnp.zeros((1, n * UNIT), F32)
    for t in range(tiles):
        top, total = lm_tile(t, top, total)
    stat_send(0, top, total)
    c_three(q, False)
    c_three(q, True)
    c_two(q)
    for k in range(q):
        c_one(k)
    for g in range(groups):
        g_end(g)
    stat_merge(0)
    c_one(q)
    for k in range(nq):
        c_end(k)
    stat_merge(1)
    for t in range(max(0, tiles - depth) if streamed else tiles, tiles):
        sc_out(t).wait()


def fused(dims, lead, heat, embed, tok, choice, router, wg, wu, wd):
    nv, ne, nx, na, nb = dims
    n = nv * ne
    local, ff, width = wg.shape
    vocab = embed.shape[0]
    rows = tok.shape[0] * UNIT
    nexp = router.shape[0]
    span = width // nv
    nq = tok.shape[0] // nv
    groups = nq + 1
    tokens = n * UNIT
    wide = -(-(width + 2 * nexp) // 128) * 128
    per = tokens // ne
    side = -(-max(2 * nexp, rows) // 128) * 128
    n1, n2, n3 = na, nb, nx
    roomy = 3 * nx * nq * tokens * (-(-span // 128) * 128) * 4 < 10 << 20
    tile = -(-vocab // (16 if roomy else 128)) * 16
    tiles = -(-vocab // tile)
    link, depth = (F32, tiles) if roomy else (BF16, 2)
    n_peers = n1 - 1 + n2 * n3 * CORES - 1
    dma = pltpu.SemaphoreType.DMA
    shape = jax.ShapeDtypeStruct if tiles > 1 else pltpu.VMEM
    kept = 0 if tiles > 1 else 2 << 20
    scratch = [
        pltpu.VMEM((vocab, width), BF16),
        pltpu.VMEM((local, ff, width), BF16),
        pltpu.VMEM((local, ff, width), BF16),
        pltpu.VMEM((2 if roomy else 1, ff, width), BF16),
        pltpu.VMEM((local, nv, ff, span), BF16),
        pltpu.VMEM(tok.shape, BF16),
        pltpu.VMEM(lead.shape, BF16),
        pltpu.VMEM(heat.shape, jnp.int32),
        pltpu.VMEM(choice.shape, jnp.int32),
        pltpu.VMEM(router.shape, BF16),
        pltpu.VMEM((side, side), F32),
        pltpu.VMEM((groups, n, UNIT, wide), BF16),
        pltpu.VMEM((tokens, width), BF16),
        pltpu.VMEM((tokens, 128), F32),
        pltpu.VMEM((local, tokens, ff), BF16),
        pltpu.VMEM((depth, tile, tokens if tiles > 1 else 128), F32),
        pltpu.VMEM((nq, nx, ne, per, span), link),
        pltpu.VMEM((nq, nx, ne, per, span), link),
        pltpu.VMEM((nq, nx, ne, per, span), link),
        pltpu.VMEM((nq, n3 - 1, n1 * n2, per, span) if roomy else (8, 128), BF16),
        pltpu.VMEM((nq, n3 - 1, n1 * n2, per, span), BF16),
        pltpu.VMEM((nq, n2 - 1, n1, per, span), BF16),
        pltpu.VMEM((nq, n2 - 1, n1, per, span), BF16),
        pltpu.VMEM((nq, n1 - 1, per, span), BF16),
        pltpu.VMEM((nq, n1 - 1, per, span), BF16),
        pltpu.VMEM((nq, n1, per, span), F32),
        pltpu.VMEM((2, 2, tokens), F32),
        pltpu.VMEM((n_peers, 2, tokens), F32),
        dma((6,)),
        dma((tiles,)),
        dma((2, local)),
        dma((local,)),
        dma((groups, n - 1)),
        dma((groups, n)),
        dma((nq, nx)),
        dma((nq, nx)),
        dma((nq, n3 - 1, n1 * n2)),
        dma((nq, n3 - 1, n1 * n2)),
        dma((nq, n2 - 1, n1)),
        dma((nq, n2 - 1, n1)),
        dma((nq, n1 - 1)),
        dma((nq, n1 - 1)),
        dma((n_peers,)),
        dma((n_peers,)),
    ]
    return pl.pallas_call(
        functools.partial(body, dims),
        out_shape=(
            shape((tiles * tile, tokens), F32),
            shape((1, tokens), F32),
            shape((rows, span), BF16),
        ),
        in_specs=[ANY] * 9,
        out_specs=(ANY if tiles > 1 else VMEM, VMEM, VMEM),
        scratch_shapes=scratch,
        compiler_params=pltpu.CompilerParams(
            collective_id=0, has_side_effects=True, vmem_limit_bytes=67043328 - kept
        ),
        name="fused",
    )(lead, heat, embed, tok, choice, router, wg, wu, wd)


def per_device(dims, lead, heat, embed, tok, choice, router, wg, wu, wd):
    scaled, norm, moe = fused(
        dims,
        lead,
        heat[None, :],
        embed,
        tok.reshape(tok.shape[0] // UNIT, UNIT, tok.shape[1]),
        choice.T,
        router.T,
        wg.swapaxes(1, 2),
        wu.swapaxes(1, 2),
        wd,
    )
    return (scaled[: embed.shape[0]] - norm).T, moe


def fast_steps(mesh, axis):
    index = mesh.axis_names.index(axis)
    devices = mesh.devices.swapaxes(0, index)[:, 0]
    places = [tuple(d.coords) for d in devices]
    moved = [i for i, (p, q) in enumerate(zip(places[0], places[1])) if p != q]
    count = 1
    while count < len(places):
        if any(p != q and i not in moved for i, (p, q) in enumerate(zip(places[0], places[count]))):
            break
        count += 1
    return count


def solution(mesh):
    nv, ne = mesh.shape["vocab"], mesh.shape["expert"]
    nb = fast_steps(mesh, "expert")
    dims = (nv, ne, nv // CORES, ne // nb, nb)
    placed = (
        P(("vocab", "expert"), None),
        P(),
        P(("vocab", "expert"), None),
        P("expert", None),
        P("expert", None),
        P(),
        P("expert", None, "vocab"),
        P("expert", None, "vocab"),
        P("expert", "vocab", None),
    )
    return jax.shard_map(
        functools.partial(per_device, dims),
        mesh=mesh,
        in_specs=placed,
        out_specs=(P(None, ("vocab", "expert")), P("expert", "vocab")),
        check_vma=False,
    )
```
